32 devices in a mesh: zero: 8 (over z, x), model: 4 (over y, core).
Axes of the slice: x: 2, y: 2, z: 4, core: 2. Of those that a mesh axis runs over, the one named last changes fastest.
Arguments:
- train_up: bfloat16 [12288, 49152], P('zero', 'model'), may hold values from -0.078125 to 0.078125
- low_up: bfloat16 [12288, 32], P('zero'), may hold values from -0.0546875 to 0.0546875
- high_up: bfloat16 [32, 49152], P(None, 'model'), may hold values from -1 to 1
- norm_train: float32 [12288], P(('zero', 'model')), may hold values from 0.25 to 1.75
- norm_step: float32 [12288], P(('zero', 'model')), may hold values from -0.3 to 0.3
Outputs:
- serving_up: bfloat16 [12288, 49152], P(None, ('model', 'zero'))
- scale_up: float32 [49152], P(('model', 'zero'))
- serve_norm: bfloat16 [12288], replicated
The draws below stay inside these ranges and needn't reach their ends.
All inputs are finite; a program needn't handle non-finite values. Where the reference program divides by a largest or mean magnitude, that divisor is 1e-20 or more.
Results may differ from the reference program's by a relative error of at most 0.001.
Values may be sent and summed in bfloat16 or wider, within the bound.
A program may use at most 192 MiB of HBM per device.

```python
import jax
import jax.numpy as jnp

D_MODEL = 12288
D_INNER = 49152
RANK = 32


def with_spikes(result, own_key, source, target, parts, factor):
    def block_of(dim):
        return (jnp.arange(result.shape[dim]) // (result.shape[dim] // parts)).reshape((-1,) + (1,) * (result.ndim - 1 - dim))

    near = jax.random.permutation(own_key, parts)[block_of(target)]
    far = (block_of(target) + parts // 2) % parts
    return jnp.where((block_of(source) == near) | (block_of(source) == far), factor * result, result)


def steps_of(rng, shape, shards, smallest, high):
    loudness, own = 1.0, jax.random.fold_in(rng, 6)
    for axis_at, parts in shards:
        draws = jnp.exp(jax.random.uniform(jax.random.fold_in(own, axis_at), (parts,), jnp.float32, smallest / len(shards), high / len(shards)))
        loudness = loudness * jnp.repeat(draws, shape[axis_at] // parts).reshape([-1 if axis == axis_at else 1 for axis in range(len(shape))])
    return loudness


def bell_draw(rng, dims, scale, limit, pieces=(), dtype=jnp.bfloat16):
    drawn = scale * jax.random.normal(rng, dims, jnp.float32)
    if pieces:
        drawn = drawn * steps_of(rng, dims, pieces, -0.22, 0.18)
    return jnp.clip(drawn, -limit, limit).astype(dtype)


def gaussian_with(key, shape, spread, reach, cuts, heavy, dtype=jnp.bfloat16):
    array = spread * jax.random.normal(key, shape, jnp.float32)
    if cuts:
        array = array * steps_of(key, shape, cuts, -0.22, 0.18)
    return jnp.clip(with_spikes(array, jax.random.fold_in(key, 3), *heavy), -reach, reach).astype(dtype)


def setup_inputs(seed: int = 0) -> dict:
    splits = jax.random.split(jax.random.key(seed), 6)
    train_up = gaussian_with(splits[0], (D_MODEL, D_INNER), D_MODEL ** -0.5, 0.078125, ((0, 8), (1, 4)), (0, 1, 8, 2.0))
    low_up = bell_draw(splits[1], (D_MODEL, RANK), D_MODEL ** -0.5, 0.0546875, ((0, 8),))
    high_up = bell_draw(splits[2], (RANK, D_INNER), RANK ** -0.5, 1.0, ((1, 4),))
    norm_train = jnp.clip(1.0 + 0.15 * jax.random.normal(splits[3], (D_MODEL,), jnp.float32), 0.25, 1.75)
    norm_step = jnp.clip(jax.random.uniform(splits[4], (D_MODEL,), jnp.float32, -0.3, 0.3) * steps_of(splits[4], (D_MODEL,), ((0, 32),), -0.4, 0.0), -0.3, 0.3)
    return {"train_up": train_up, "low_up": low_up, "high_up": high_up, "norm_train": norm_train, "norm_step": norm_step}


mix_rate = 0.5


def reference(train_up, low_up, high_up, norm_train, norm_step):
    whole_up = train_up.astype(jnp.float32) + mix_rate * jnp.dot(low_up, high_up, preferred_element_type=jnp.float32)
    scale_up = jnp.sum(jnp.abs(whole_up), axis=0) / D_MODEL
    serving_up = (whole_up / scale_up).astype(jnp.bfloat16)
    serve_norm = (norm_train + norm_step).astype(jnp.bfloat16)
    return serving_up, scale_up, serve_norm
```

```python
import functools

import jax
import jax.numpy as jnp
from jax import lax
from jax.experimental import pallas as pl
from jax.experimental.pallas import tpu as pltpu
from jax.sharding import PartitionSpec as P

mix_rate = 0.5
PIECES = 4


def partner(me, bits, n):
    other, place = me, 1
    while place < n:
        if (bits // place) % 2:
            other = other + place * (1 - 2 * (lax.div(me, place) % 2))
        place *= 2
    return other


def send_order(n):
    far = [k for k in range(n // 2, n)]
    near = [k for k in range(n // 2 - 1, 0, -1)]
    order = []
    for i in range(len(far)):
        order.append(far[i])
        if i < len(near):
            order.append(near[i])
    return order


def exchange(n, pieces, train, low, landed, lows, own, own_low, sends, recvs, low_sends, low_recvs, mine):
    me = lax.axis_index("zero")
    rows = train.shape[0]
    cols = landed.shape[1]
    step = rows // pieces
    order = send_order(n)

    barrier = pltpu.get_barrier_semaphore()
    for k in order:
        pl.semaphore_signal(barrier, inc=1, device_id={"zero": partner(me, k, n)}, device_id_type=pl.DeviceIdType.MESH)
    pl.semaphore_wait(barrier, n - 1)

    copies = []
    for piece in range(pieces):
        for k in order:
            dest = partner(me, k, n)
            copy = pltpu.make_async_remote_copy(
                src_ref=train.at[pl.ds(piece * step, step), pl.ds(pl.multiple_of(dest * cols, 128), cols)],
                dst_ref=landed.at[pl.ds(pl.multiple_of(me * rows + piece * step, 16), step), :],
                send_sem=sends.at[k, piece],
                recv_sem=recvs.at[k, piece],
                device_id={"zero": dest},
                device_id_type=pl.DeviceIdType.MESH,
            )
            copy.start()
            copies.append(copy)
        if piece == 0:
            for k in order:
                copy = pltpu.make_async_remote_copy(
                    src_ref=low,
                    dst_ref=lows.at[me],
                    send_sem=low_sends.at[k],
                    recv_sem=low_recvs.at[k],
                    device_id={"zero": partner(me, k, n)},
                    device_id_type=pl.DeviceIdType.MESH,
                )
                copy.start()
                copies.append(copy)

    fetch = pltpu.make_async_copy(train.at[:, pl.ds(pl.multiple_of(me * cols, 128), cols)], own, mine.at[0])
    fetch_low = pltpu.make_async_copy(low, own_low, mine.at[1])
    fetch.start()
    fetch_low.start()
    fetch.wait()
    fetch_low.wait()
    keep = pltpu.make_async_copy(own, landed.at[pl.ds(pl.multiple_of(me * rows, 16), rows), :], mine.at[2])
    keep_low = pltpu.make_async_copy(own_low, lows.at[me], mine.at[3])
    keep.start()
    keep_low.start()
    keep.wait()
    keep_low.wait()
    for copy in copies:
        copy.wait()


def gather_blocks(n, train, low):
    rows, width = train.shape
    cols = width // n
    return pl.pallas_call(
        functools.partial(exchange, n, PIECES),
        out_shape=(
            jax.ShapeDtypeStruct((n * rows, cols), train.dtype),
            jax.ShapeDtypeStruct((n,) + low.shape, low.dtype),
        ),
        in_specs=[pl.BlockSpec(memory_space=pl.ANY)] * 2,
        out_specs=[pl.BlockSpec(memory_space=pl.ANY)] * 2,
        scratch_shapes=[
            pltpu.VMEM((rows, cols), train.dtype),
            pltpu.VMEM(low.shape, low.dtype),
            pltpu.SemaphoreType.DMA((n, PIECES)),
            pltpu.SemaphoreType.DMA((n, PIECES)),
            pltpu.SemaphoreType.DMA((n,)),
            pltpu.SemaphoreType.DMA((n,)),
            pltpu.SemaphoreType.DMA((4,)),
        ],
        compiler_params=pltpu.CompilerParams(collective_id=0, has_side_effects=True, vmem_limit_bytes=60 * 2**20),
        name="exchange",
    )(train, low)


def normalise(tall, landed, lows, high, serving, scale, whole):
    n, _, rows = lows.shape
    width = landed.shape[1]
    per = rows // tall
    high_tile = high[...]

    def add_up(t, total):
        i, j = lax.div(t, per), lax.rem(t, per)
        at = pl.multiple_of(t * tall, tall)
        low = lows[i, :, pl.ds(pl.multiple_of(j * tall, 128), tall)]
        extra = lax.dot_general(low, high_tile, (((0,), (0,)), ((), ())), preferred_element_type=jnp.float32)
        w = landed[pl.ds(at, tall), :].astype(jnp.float32) + extra
        whole[pl.ds(at, tall), :] = w
        return total + jnp.sum(jnp.abs(w).reshape(tall // 8, 8, width), axis=0)

    total = lax.fori_loop(0, n * per, add_up, jnp.zeros((8, width), jnp.float32), unroll=2)
    mean = jnp.sum(total, axis=0, keepdims=True) / (n * rows)
    scale[...] = mean
    inverse = 1.0 / mean

    def divide(t, carry):
        at = pl.multiple_of(t * tall, tall)
        serving[pl.ds(at, tall), :] = (whole[pl.ds(at, tall), :] * inverse).astype(serving.dtype)
        return carry

    lax.fori_loop(0, n * per, divide, 0, unroll=2)


def serve(landed, lows, high):
    height, cols = landed.shape
    n, rank, rows = lows.shape
    width = 256 if cols % 256 == 0 else 128
    tall = 256 if rows % 256 == 0 else 128
    return pl.pallas_call(
        functools.partial(normalise, tall),
        grid=(cols // width,),
        out_shape=(
            jax.ShapeDtypeStruct((height, cols), jnp.bfloat16),
            jax.ShapeDtypeStruct((1, cols), jnp.float32),
        ),
        in_specs=[
            pl.BlockSpec((height, width), lambda c: (0, c)),
            pl.BlockSpec((n, rank, rows), lambda c: (0, 0, 0)),
            pl.BlockSpec((rank, width), lambda c: (0, c)),
        ],
        out_specs=[
            pl.BlockSpec((height, width), lambda c: (0, c)),
            pl.BlockSpec((1, width), lambda c: (0, c)),
        ],
        scratch_shapes=[pltpu.VMEM((height, width), jnp.float32)],
        compiler_params=pltpu.CompilerParams(vmem_limit_bytes=60 * 2**20, dimension_semantics=("arbitrary",)),
        name="serve",
    )(landed, lows, high)


def local(n, train_up, low_up, high_up, norm_train, norm_step):
    serve_norm = lax.all_gather(
        (norm_train + norm_step).astype(jnp.bfloat16), ("zero", "model"), axis=0, tiled=True
    )
    cols = train_up.shape[1] // n
    high = lax.dynamic_slice_in_dim(high_up, lax.axis_index("zero") * cols, cols, axis=1)
    high = (mix_rate * high.astype(jnp.float32)).astype(jnp.bfloat16)
    landed, lows = gather_blocks(n, train_up, low_up.T)
    serving_up, scale_up = serve(landed, lows, high)
    return (serving_up, scale_up.reshape(-1), serve_norm)


def solution(mesh):
    in_specs = (
        P("zero", "model"),
        P("zero", None),
        P(None, "model"),
        P(("zero", "model")),
        P(("zero", "model")),
    )
    out_specs = (P(None, ("model", "zero")), P(("model", "zero")), P())
    body = functools.partial(local, mesh.shape["zero"])
    return jax.shard_map(body, mesh=mesh, in_specs=in_specs, out_specs=out_specs, check_vma=False)
```

```python
import functools

import jax
import jax.numpy as jnp
from jax import lax
from jax.experimental import pallas as pl
from jax.experimental.pallas import tpu as pltpu
from jax.sharding import PartitionSpec as P

mix_rate = 0.5
PIECES = 4


def partner(me, bits, n):
    other, place = me, 1
    while place < n:
        if (bits // place) % 2:
            other = other + place * (1 - 2 * (lax.div(me, place) % 2))
        place *= 2
    return other


def send_order(n):
    far = [k for k in range(n // 2, n)]
    near = [k for k in range(n // 2 - 1, 0, -1)]
    order = []
    for i in range(len(far)):
        order.append(far[i])
        if i < len(near):
            order.append(near[i])
    return order


def exchange(n, pieces, train, low, norm, landed, lows, norms, own, own_low, own_norm, sends, recvs, low_sends, low_recvs, norm_sends, norm_recvs, mine):
    me = lax.axis_index("zero")
    rows = train.shape[0]
    cols = landed.shape[1]
    step = rows // pieces
    order = send_order(n)

    barrier = pltpu.get_barrier_semaphore()
    for k in order:
        pl.semaphore_signal(barrier, inc=1, device_id={"zero": partner(me, k, n)}, device_id_type=pl.DeviceIdType.MESH)
    pl.semaphore_wait(barrier, n - 1)

    copies = []
    for piece in range(pieces):
        for k in order:
            dest = partner(me, k, n)
            copy = pltpu.make_async_remote_copy(
                src_ref=train.at[pl.ds(piece * step, step), pl.ds(pl.multiple_of(dest * cols, 128), cols)],
                dst_ref=landed.at[pl.ds(pl.multiple_of(me * rows + piece * step, 16), step), :],
                send_sem=sends.at[k, piece],
                recv_sem=recvs.at[k, piece],
                device_id={"zero": dest},
                device_id_type=pl.DeviceIdType.MESH,
            )
            copy.start()
            copies.append(copy)
        if piece == 0:
            for k in order:
                copy = pltpu.make_async_remote_copy(
                    src_ref=low,
                    dst_ref=lows.at[me],
                    send_sem=low_sends.at[k],
                    recv_sem=low_recvs.at[k],
                    device_id={"zero": partner(me, k, n)},
                    device_id_type=pl.DeviceIdType.MESH,
                )
                copy.start()
                copies.append(copy)
                copy = pltpu.make_async_remote_copy(
                    src_ref=norm,
                    dst_ref=norms.at[me],
                    send_sem=norm_sends.at[k],
                    recv_sem=norm_recvs.at[k],
                    device_id={"zero": partner(me, k, n)},
                    device_id_type=pl.DeviceIdType.MESH,
                )
                copy.start()
                copies.append(copy)

    fetch = pltpu.make_async_copy(train.at[:, pl.ds(pl.multiple_of(me * cols, 128), cols)], own, mine.at[0])
    fetch_low = pltpu.make_async_copy(low, own_low, mine.at[1])
    fetch_norm = pltpu.make_async_copy(norm, own_norm, mine.at[4])
    fetch_norm.start()
    fetch.start()
    fetch_low.start()
    fetch.wait()
    fetch_low.wait()
    fetch_norm.wait()
    keep = pltpu.make_async_copy(own, landed.at[pl.ds(pl.multiple_of(me * rows, 16), rows), :], mine.at[2])
    keep_low = pltpu.make_async_copy(own_low, lows.at[me], mine.at[3])
    keep_norm = pltpu.make_async_copy(own_norm, norms.at[me], mine.at[5])
    keep_norm.start()
    keep.start()
    keep_low.start()
    keep.wait()
    keep_low.wait()
    keep_norm.wait()
    for copy in copies:
        copy.wait()


def gather_blocks(n, train, low, norm):
    rows, width = train.shape
    cols = width // n
    return pl.pallas_call(
        functools.partial(exchange, n, PIECES),
        out_shape=(
            jax.ShapeDtypeStruct((n * rows, cols), train.dtype),
            jax.ShapeDtypeStruct((n,) + low.shape, low.dtype),
            jax.ShapeDtypeStruct((n,) + norm.shape, norm.dtype),
        ),
        in_specs=[pl.BlockSpec(memory_space=pl.ANY)] * 3,
        out_specs=[pl.BlockSpec(memory_space=pl.ANY)] * 3,
        scratch_shapes=[
            pltpu.VMEM((rows, cols), train.dtype),
            pltpu.VMEM(low.shape, low.dtype),
            pltpu.VMEM(norm.shape, norm.dtype),
            pltpu.SemaphoreType.DMA((n, PIECES)),
            pltpu.SemaphoreType.DMA((n, PIECES)),
            pltpu.SemaphoreType.DMA((n,)),
            pltpu.SemaphoreType.DMA((n,)),
            pltpu.SemaphoreType.DMA((n,)),
            pltpu.SemaphoreType.DMA((n,)),
            pltpu.SemaphoreType.DMA((6,)),
        ],
        compiler_params=pltpu.CompilerParams(collective_id=0, has_side_effects=True, vmem_limit_bytes=60 * 2**20),
        name="exchange",
    )(train, low, norm)


def normalise(tall, landed, lows, high, serving, scale, whole):
    n, _, rows = lows.shape
    width = landed.shape[1]
    per = rows // tall
    high_tile = high[...]

    def add_up(t, total):
        i, j = lax.div(t, per), lax.rem(t, per)
        at = pl.multiple_of(t * tall, tall)
        low = lows[i, :, pl.ds(pl.multiple_of(j * tall, 128), tall)]
        extra = lax.dot_general(low, high_tile, (((0,), (0,)), ((), ())), preferred_element_type=jnp.float32)
        w = landed[pl.ds(at, tall), :].astype(jnp.float32) + extra
        whole[pl.ds(at, tall), :] = w
        return total + jnp.sum(jnp.abs(w).reshape(tall // 8, 8, width), axis=0)

    total = lax.fori_loop(0, n * per, add_up, jnp.zeros((8, width), jnp.float32), unroll=4)
    mean = jnp.sum(total, axis=0, keepdims=True) / (n * rows)
    scale[...] = mean
    inverse = 1.0 / mean

    def divide(t, carry):
        at = pl.multiple_of(t * tall, tall)
        serving[pl.ds(at, tall), :] = (whole[pl.ds(at, tall), :] * inverse).astype(serving.dtype)
        return carry

    lax.fori_loop(0, n * per, divide, 0, unroll=2)


def serve(landed, lows, high):
    height, cols = landed.shape
    n, rank, rows = lows.shape
    width = 256 if cols % 256 == 0 else 128
    tall = 256 if rows % 256 == 0 else 128
    return pl.pallas_call(
        functools.partial(normalise, tall),
        grid=(cols // width,),
        out_shape=(
            jax.ShapeDtypeStruct((height, cols), jnp.bfloat16),
            jax.ShapeDtypeStruct((1, cols), jnp.float32),
        ),
        in_specs=[
            pl.BlockSpec((height, width), lambda c: (0, c)),
            pl.BlockSpec((n, rank, rows), lambda c: (0, 0, 0)),
            pl.BlockSpec((rank, width), lambda c: (0, c)),
        ],
        out_specs=[
            pl.BlockSpec((height, width), lambda c: (0, c)),
            pl.BlockSpec((1, width), lambda c: (0, c)),
        ],
        scratch_shapes=[pltpu.VMEM((height, width), jnp.float32)],
        compiler_params=pltpu.CompilerParams(vmem_limit_bytes=60 * 2**20, dimension_semantics=("arbitrary",)),
        name="serve",
    )(landed, lows, high)


def local(n, train_up, low_up, high_up, norm_train, norm_step):
    norm = lax.all_gather(norm_train + norm_step, "model", axis=0, tiled=True).reshape(1, -1)
    cols = train_up.shape[1] // n
    high = lax.dynamic_slice_in_dim(high_up, lax.axis_index("zero") * cols, cols, axis=1)
    high = (mix_rate * high.astype(jnp.float32)).astype(jnp.bfloat16)
    landed, lows, norms = gather_blocks(n, train_up, low_up.T, norm)
    serve_norm = norms.reshape(-1).astype(jnp.bfloat16)
    serving_up, scale_up = serve(landed, lows, high)
    return (serving_up, scale_up.reshape(-1), serve_norm)


def solution(mesh):
    in_specs = (
        P("zero", "model"),
        P("zero", None),
        P(None, "model"),
        P(("zero", "model")),
        P(("zero", "model")),
    )
    out_specs = (P(None, ("model", "zero")), P(("model", "zero")), P())
    body = functools.partial(local, mesh.shape["zero"])
    return jax.shard_map(body, mesh=mesh, in_specs=in_specs, out_specs=out_specs, check_vma=False)
```
